32 devices in a mesh: section: 2 (over y), expert: 2 (over x), tensor: 8 (over z, core).
Axes of the slice: x: 2, y: 2, z: 4, core: 2. Of those that a mesh axis runs over, the one named last changes fastest.
Arguments:
- query: bfloat16 [2, 512, 4096], P('expert', 'tensor', 'section'), may hold values from -24 to 24
- keys: bfloat16 [2, 512, 1024], P('expert', 'tensor', 'section'), may hold values from -24 to 24
- values: bfloat16 [2, 512, 1024], P('expert', 'tensor', 'section'), may hold values from -6 to 6
- residual: bfloat16 [2, 512, 4096], P('expert', 'tensor', 'section'), may hold values from -6 to 6
- routes: int32 [2, 512, 2], P('expert', 'tensor'), may hold values from 0 to 7, all different within a row; in each aligned block of 64 rows (0 to 63, 64 to 127, ..., all dimensions but the last counted through in order) at most 17 rows name the same one
- gates: float32 [2, 512, 2], P('expert', 'tensor'), may hold values from 0.1 to 0.9
- w_gate: bfloat16 [8, 4096, 8192], P('expert', None, 'tensor'), may hold values from -0.09375 to 0.09375
- w_up: bfloat16 [8, 4096, 8192], P('expert', None, 'tensor'), may hold values from -0.09375 to 0.09375
- w_down: bfloat16 [8, 8192, 4096], P('expert', 'tensor'), may hold values from -0.0625 to 0.0625
Outputs:
- layer_out: bfloat16 [2, 512, 4096], P('expert', 'tensor', 'section')
The draws below stay inside these ranges and needn't reach their ends.
Inputs may be any that keep to these rules, and one draw needn't show every extreme that they name: `routes`: the 2 entries of a row differ. In the rows of one index of expert and tensor (aligned blocks of 64 positions, taken in order over sequences and positions) no expert is named more than 17 times.
All inputs are finite; a program needn't handle non-finite values.
Results may differ from the reference program's by a relative error of at most 0.014.
Values may be sent and summed in bfloat16 or wider, within the bound.
No kernel may reach another device: no remote copies, remote signals or barrier semaphores. Data moves between devices by JAX's collectives and lax.ppermute only.
A program may use at most 192 MiB of HBM per device.

```python
import math
import jax
import jax.numpy as jnp
import numpy as np
from jax import lax

D = 4096
H = 32
KVH = 8
HD = 128
EXPERTS = 8
TOP = 2
FF = 8192
TOK_DEV = 64
CAP = 17
GROUPS = 8
SEQS = 2
LENGTH = 512
N_EXPERT = 2
N_TENSOR = 8


def attention_pair(key):
    key_noise = jnp.clip(jax.random.normal(jax.random.fold_in(key, 11), (SEQS, LENGTH, KVH * HD), jnp.float32), -4.5, 4.5)
    query_noise = jnp.clip(jax.random.normal(jax.random.fold_in(key, 12), (SEQS, LENGTH, H * HD), jnp.float32), -4.5, 4.5)
    key_field = key_noise
    query_field = query_noise
    return (query_field, key_field)


def draw_query(key, part):
    return attention_pair(key)[0].astype(jnp.bfloat16)


def draw_keys(key, part):
    return attention_pair(key)[1].astype(jnp.bfloat16)


def block_scale(stream_key, shape, pieces, low, high):
    level, own = 1.0, jax.random.fold_in(stream_key, 6)
    for axis_at, parts in pieces:
        heights = jnp.exp(jax.random.uniform(jax.random.fold_in(own, axis_at), (parts,), jnp.float32, low / len(pieces), high / len(pieces)))
        level = level * jnp.repeat(heights, shape[axis_at] // parts).reshape([-1 if axis == axis_at else 1 for axis in range(len(shape))])
    return level


def deal_out(rng, own, number, rows, amount, top, reach, slope):
    ranking = jax.random.permutation(rng, amount)
    crowded, common = portions_of(amount, rows * top, reach, slope, True), portions_of(amount, rows * top, reach, slope, False)
    places = jnp.arange(amount)

    def named(tallies, rotation):
        used = int((tallies > 0).sum())
        fixed = max(1, used // 4)
        moved = fixed + (places - fixed + rotation * (used - fixed)) % max(1, amount - fixed)
        return jnp.zeros((amount,), jnp.int32).at[ranking[jnp.where(places < fixed, places, moved)]].set(jnp.asarray(tallies, jnp.int32))

    tallies = jnp.where(number % 4 == 0, named(crowded, number // 4), named(common, number - number // 4 - 1))
    mixed = jax.random.permutation(jax.random.fold_in(own, 3), amount)
    donor, sink = mixed[0:amount // 2 * 2:2], mixed[1:amount // 2 * 2:2]
    slack = jnp.minimum(tallies[donor] - 1, reach - tallies[sink]) // 2
    slack = jnp.where((donor == ranking[0]) | (sink == ranking[0]) | (tallies[sink] == 0), 0, jnp.maximum(slack, 0))
    moved = jax.random.randint(jax.random.fold_in(own, 4), (amount // 2,), 0, 1 << 20) % (slack + 1)
    tallies = tallies.at[donor].add(-moved).at[sink].add(moved)
    labels = jnp.searchsorted(jnp.cumsum(tallies), jnp.arange(rows * top), side="right").astype(jnp.int32)
    listing = labels.reshape(top, rows).T
    listing = listing[jax.random.permutation(jax.random.fold_in(own, 1), rows)]
    rotation = jax.random.randint(jax.random.fold_in(own, 2), (rows, 1), 0, top)
    return jnp.take_along_axis(listing, (jnp.arange(top)[None, :] + rotation) % top, axis=1)


def portions_of(number_of, total, most, skew, full):
    loads = [(1 << 20) // math.isqrt(standing ** skew) + 1 for standing in range(1, number_of + 1)]
    largest = most if full else min(most, max(-(-total // number_of), total * loads[0] // sum(loads)))
    least = 1 if total - largest >= number_of - 1 else 0
    counts, surplus = [largest] + [least] * (number_of - 1), total - largest - least * (number_of - 1)
    while surplus > 0:
        candidates = [i for i in range(1, number_of) if counts[i] < largest] or [i for i in range(1, number_of) if counts[i] < most]
        pool, remaining = sum([loads[i] for i in candidates]), surplus
        for i in candidates:
            more = min(most - counts[i], max(1, remaining * loads[i] // pool), surplus)
            counts[i] = counts[i] + more
            surplus = surplus - more
    return np.array(counts)


def gaussian(own_key, dims, scale, bound, shards=(), held_as=jnp.bfloat16):
    factor_of = block_scale(own_key, dims, shards, -0.22, 0.18) if shards else 1.0
    array = jax.random.normal(own_key, dims, jnp.float32) * scale * factor_of
    return jnp.minimum(jnp.maximum(array, -bound), bound).astype(held_as)


def setup_inputs(seed: int = 0) -> dict:
    seeds = jax.random.split(jax.random.key(seed), 10)
    query = draw_query(jax.random.fold_in(seeds[9], 71), 0)
    keys = draw_keys(jax.random.fold_in(seeds[9], 71), 0)
    values = gaussian(seeds[2], (SEQS, LENGTH, KVH * HD), 1.0, 6.0, ((0, 2), (1, 8), (2, 2)))
    residual = gaussian(seeds[3], (SEQS, LENGTH, D), 1.0, 6.0, ((0, 2), (1, 8), (2, 2)))
    routes_keys = jax.random.split(jax.random.fold_in(seeds[4], 1), SEQS * LENGTH // TOK_DEV)
    routes_turns = jax.random.permutation(jax.random.fold_in(seeds[4], 3), SEQS * LENGTH // TOK_DEV)
    routes = jax.vmap(lambda own, number: deal_out(jax.random.fold_in(seeds[4], 2), own, number, TOK_DEV, EXPERTS, TOP, CAP, 2))(routes_keys, routes_turns).reshape((SEQS, LENGTH, TOP))
    gates = jnp.clip(0.1 + 0.79999997 * jax.random.uniform(seeds[5], (SEQS, LENGTH, TOP), jnp.float32) ** block_scale(seeds[5], (SEQS, LENGTH, TOP), ((0, 2), (1, 8)), -0.2, 0.2), 0.1, 0.9)
    w_gate = gaussian(seeds[6], (EXPERTS, D, FF), D ** -0.5, 0.09375, ((0, 2), (2, 8)))
    w_up = gaussian(seeds[7], (EXPERTS, D, FF), D ** -0.5, 0.09375, ((0, 2), (2, 8)))
    w_down = gaussian(seeds[8], (EXPERTS, FF, D), FF ** -0.5, 0.0625, ((0, 2), (1, 8)))
    return dict(query=query, keys=keys, values=values, residual=residual, routes=routes, gates=gates, w_gate=w_gate, w_up=w_up, w_down=w_down)


def attend(query_seq, key_seq, value_seq):
    length = query_seq.shape[0]
    groups = H // KVH
    queries = query_seq.reshape(length, KVH, groups, HD).astype(jnp.float32)
    keys_all = key_seq.reshape(length, KVH, HD).astype(jnp.float32)
    values_all = value_seq.reshape(length, KVH, HD).astype(jnp.float32)
    scores = jnp.einsum('qkgd,tkd->kgqt', queries, keys_all) / math.sqrt(HD)
    positions = jnp.arange(length)
    causal = positions[:, None] >= positions[None, :]
    masked = jnp.where(causal, scores, -1e+30)
    row_peak = lax.optimization_barrier(jnp.max(masked, axis=-1, keepdims=True))
    exp_terms = jnp.where(causal, jnp.exp(masked - row_peak), 0.0)
    weights = (exp_terms / lax.optimization_barrier(jnp.sum(exp_terms, axis=-1, keepdims=True))).astype(jnp.bfloat16)
    context = jnp.einsum('kgqt,tkd->qkgd', weights.astype(jnp.float32), values_all)
    return context.reshape(length, H * HD)

def reference(query, keys, values, residual, routes, gates, w_gate, w_up, w_down):
    context = lax.map(lambda triple: attend(triple[0], triple[1], triple[2]), (query, keys, values))
    hidden = (residual.astype(jnp.float32) + context).astype(jnp.bfloat16)
    token_total = SEQS * LENGTH
    hidden_flat = hidden.reshape(token_total, D)
    picked = routes.reshape(token_total * TOP).astype(jnp.int32)
    most_rows = CAP * N_EXPERT * N_TENSOR
    block_count = GROUPS
    block_width = FF // block_count

    def expert_pass(expert_id, outputs):
        matches = jnp.nonzero(picked == expert_id, size=most_rows, fill_value=token_total * TOP)[0].astype(jnp.int32)
        safe_index = jnp.minimum(matches, token_total * TOP - 1)
        token_rows = hidden_flat[safe_index // TOP]
        gate_part = jnp.dot(token_rows, w_gate[expert_id], preferred_element_type=jnp.float32)
        up_part = jnp.dot(token_rows, w_up[expert_id], preferred_element_type=jnp.float32)
        inner_rows = (jax.nn.silu(gate_part) * up_part).astype(jnp.bfloat16)
        down_full = w_down[expert_id]

        def add_block(block_id, running):
            inner_block = lax.dynamic_slice_in_dim(inner_rows, block_id * block_width, block_width, 1)
            down_block = lax.dynamic_slice_in_dim(down_full, block_id * block_width, block_width, 0)
            partial_value = jnp.dot(inner_block, down_block, preferred_element_type=jnp.float32).astype(jnp.bfloat16)
            return running + partial_value.astype(jnp.float32)
        summed = lax.fori_loop(0, block_count, add_block, jnp.zeros((most_rows, D), jnp.float32))
        return outputs.at[matches].set(summed.astype(jnp.bfloat16), mode='drop')
    expert_out = lax.fori_loop(0, EXPERTS, expert_pass, jnp.zeros((token_total * TOP, D), jnp.bfloat16))
    weighted = gates.reshape(token_total, TOP, 1).astype(jnp.float32) * expert_out.reshape(token_total, TOP, D).astype(jnp.float32)
    layer_out = hidden_flat.astype(jnp.float32) + lax.optimization_barrier(jnp.sum(weighted, axis=1))
    return layer_out.astype(jnp.bfloat16).reshape(SEQS, LENGTH, D)
```

```python
import functools
import math

import jax
import jax.numpy as jnp
from jax import lax
from jax.experimental import pallas as pl
from jax.experimental.pallas import tpu as pltpu
from jax.sharding import PartitionSpec as P

HD = 128
EXPERTS = 8
TOP = 2
CAP = 17
META = 128
BF = jnp.bfloat16
F32 = jnp.float32


def swap(value, axis, mask):
    pairs = [(i, i ^ mask) for i in range(lax.axis_size(axis))]
    return lax.ppermute(value, axis, pairs)


def bits_of(axis, lowest):
    count = lax.axis_size(axis).bit_length() - 1
    return [(axis, 1 << b) for b in reversed(range(lowest, count))]


def gather_steps():
    return bits_of("tensor", 1) + bits_of("expert", 0) + [("tensor", 1)]


def gather_all(block, steps):
    for axis, mask in steps:
        block = jnp.concatenate([block, swap(block, axis, mask)], axis=0)
    return block


def scatter_sum(total, steps):
    for axis, mask in reversed(steps):
        half = total.shape[0] // 2
        arrived = swap(total[half:], axis, mask)
        total = (total[:half].astype(F32) + arrived.astype(F32)).astype(BF)
    return total


def hot_rows(rank_row, first, count):
    slots = lax.broadcasted_iota(jnp.int32, (count, rank_row.shape[1]), 0) + first
    return slots == rank_row


def inner_kernel(
    scal, x_own, x_oth, rank, wg_own, wg_oth, wu_own, wu_oth, out, rows_own, rows_oth, *, main, cap
):
    e, n = pl.program_id(0), pl.program_id(1)
    rank_row = rank[pl.ds(e, 1), :]

    def part(first, count):
        @pl.when(n == 0)
        def _():
            hot = hot_rows(rank_row, first, count).astype(BF)
            for src, dst in ((x_own, rows_own), (x_oth, rows_oth)):
                dst[first : first + count, :] = jnp.dot(
                    hot, src[...], preferred_element_type=F32
                ).astype(BF)

        mine = rows_own[first : first + count, :]
        rest = rows_oth[first : first + count, :]
        gate = jnp.dot(mine, wg_own[0], preferred_element_type=F32) + jnp.dot(
            rest, wg_oth[0], preferred_element_type=F32
        )
        up = jnp.dot(mine, wu_own[0], preferred_element_type=F32) + jnp.dot(
            rest, wu_oth[0], preferred_element_type=F32
        )
        out[0, first : first + count, :] = (gate / (1.0 + jnp.exp(-gate)) * up).astype(BF)

    part(0, main)
    if cap > main:

        @pl.when(scal[1 + e] > main)
        def _():
            part(main, cap - main)


def expert_inner(scal, x_own, x_oth, rank, w_gate, w_up, main, cap):
    experts, width, hidden = w_gate.shape
    half, tokens = width // 2, x_oth.shape[0]
    block = min(256, hidden)
    own = pl.BlockSpec((1, half, block), lambda e, n, s: (e, s[0], n))
    oth = pl.BlockSpec((1, half, block), lambda e, n, s: (e, 1 - s[0], n))
    return pl.pallas_call(
        functools.partial(inner_kernel, main=main, cap=cap),
        grid_spec=pltpu.PrefetchScalarGridSpec(
            num_scalar_prefetch=1,
            grid=(experts, hidden // block),
            in_specs=[
                pl.BlockSpec((tokens, half), lambda e, n, s: (0, 0)),
                pl.BlockSpec((tokens, half), lambda e, n, s: (0, 0)),
                pl.BlockSpec((experts, tokens), lambda e, n, s: (0, 0)),
                own,
                oth,
                own,
                oth,
            ],
            out_specs=pl.BlockSpec((1, cap, block), lambda e, n, s: (e, 0, n)),
            scratch_shapes=[pltpu.VMEM((cap, half), BF), pltpu.VMEM((cap, half), BF)],
        ),
        out_shape=jax.ShapeDtypeStruct((experts, cap, hidden), BF),
        cost_estimate=pl.CostEstimate(
            flops=4 * experts * main * width * hidden,
            bytes_accessed=4 * experts * width * hidden,
            transcendentals=experts * main * hidden,
        ),
        name="inner",
    )(scal, x_own, x_oth, rank, w_gate, w_gate, w_up, w_up)


def outer_kernel(scal, inner, rank, rank_t, gate, wd, out, hot, hot_t, slot_gate, total, *, main, cap):
    experts = wd.shape[0]
    tokens = rank.shape[1]

    def prepare(e, first, count):
        marks = hot_rows(rank[e : e + 1, :], first, count)
        slot_gate[e, first : first + count, :] = jnp.sum(
            jnp.where(marks, gate[e : e + 1, :], 0.0), axis=1, keepdims=True
        )
        lanes = lax.broadcasted_iota(jnp.int32, (tokens, count), 1) + first
        return (lanes == rank_t[:, e : e + 1]).astype(BF)

    def product(e, first, count):
        value = jnp.dot(inner[e, first : first + count, :], wd[e], preferred_element_type=F32)
        return (value * slot_gate[e, first : first + count, :]).astype(BF)

    @pl.when(pl.program_id(0) == 0)
    def _():
        for e in range(experts):
            hot[:, e * main : (e + 1) * main] = prepare(e, 0, main)

    sums = jnp.concatenate([product(e, 0, main) for e in range(experts)], axis=0)
    total[...] = jnp.dot(hot[...], sums, preferred_element_type=F32)
    if cap > main:
        for e in range(experts):

            @pl.when(scal[1 + e] > main)
            def _():
                hot_t[...] = prepare(e, main, cap - main)
                total[...] += jnp.dot(
                    hot_t[...], product(e, main, cap - main), preferred_element_type=F32
                )

    out[...] = total[...].astype(BF)


def expert_outer(scal, inner, rank, rank_t, gate, w_down, other, main, cap):
    experts, hidden, width = w_down.shape
    half, tokens = width // 2, rank.shape[1]
    block = min(256, half)
    blocks = half // block
    if other:
        where = lambda n, s: (0, 0, (1 - s[0]) * blocks + n)
    else:
        where = lambda n, s: (0, 0, s[0] * blocks + n)
    return pl.pallas_call(
        functools.partial(outer_kernel, main=main, cap=cap),
        grid_spec=pltpu.PrefetchScalarGridSpec(
            num_scalar_prefetch=1,
            grid=(blocks,),
            in_specs=[
                pl.BlockSpec((experts, cap, hidden), lambda n, s: (0, 0, 0)),
                pl.BlockSpec((experts, tokens), lambda n, s: (0, 0)),
                pl.BlockSpec((tokens, experts), lambda n, s: (0, 0)),
                pl.BlockSpec((experts, tokens), lambda n, s: (0, 0)),
                pl.BlockSpec((experts, hidden, block), where),
            ],
            out_specs=pl.BlockSpec((tokens, block), lambda n, s: (0, n)),
            scratch_shapes=[
                pltpu.VMEM((tokens, experts * main), BF),
                pltpu.VMEM((tokens, max(cap - main, 8)), BF),
                pltpu.VMEM((experts, cap, 1), F32),
                pltpu.VMEM((tokens, block), F32),
            ],
        ),
        out_shape=jax.ShapeDtypeStruct((tokens, half), BF),
        cost_estimate=pl.CostEstimate(
            flops=2 * experts * main * (hidden + tokens) * half,
            bytes_accessed=2 * experts * hidden * half,
            transcendentals=0,
        ),
        name="outer",
    )(scal, inner, rank, rank_t, gate, w_down)


def wide_experts(section, x_own, x_oth, rank, gate, w_gate, w_up, w_down, cap):
    half = x_oth.shape[1]
    first = section == 0
    rows = jnp.concatenate(
        [jnp.where(first, x_own, x_oth), jnp.where(first, x_oth, x_own)], axis=1
    )
    tokens, width = rows.shape
    total = jnp.zeros((tokens, width), F32)
    for e in range(w_gate.shape[0]):
        hot = hot_rows(rank[e : e + 1, :], 0, cap)
        slot_gate = jnp.sum(jnp.where(hot, gate[e : e + 1, :], 0.0), axis=1, keepdims=True)
        hot = hot.astype(BF)
        picked = jnp.dot(hot, rows, preferred_element_type=F32).astype(BF)
        g = jnp.dot(picked, w_gate[e], preferred_element_type=F32)
        u = jnp.dot(picked, w_up[e], preferred_element_type=F32)
        inner = (jax.nn.silu(g) * u).astype(BF)
        value = jnp.dot(inner, w_down[e], preferred_element_type=F32)
        value = (value * slot_gate).astype(BF)
        total = total + jnp.dot(hot.T, value, preferred_element_type=F32)
    total = total.astype(BF)
    own = lax.dynamic_slice_in_dim(total, section * half, half, 1)
    oth = lax.dynamic_slice_in_dim(total, (1 - section) * half, half, 1)
    return own, oth


def attention(query, keys, values, residual):
    token_count, half_width = query.shape
    kv_width = keys.shape[1]
    both = jnp.concatenate([keys, values], axis=1)
    steps = bits_of("tensor", 0)
    both = gather_all(both, steps)
    length = both.shape[0]
    me = lax.axis_index("tensor")
    order = jnp.zeros((1,), jnp.int32)
    for axis, mask in steps:
        order = jnp.concatenate([order, order ^ mask])
    source = me ^ order
    key_positions = (source[:, None] * token_count + jnp.arange(token_count)[None, :]).reshape(-1)
    local_kv = kv_width // HD
    groups = half_width // kv_width
    queries = query.reshape(token_count, local_kv, groups, HD)
    key_heads = both[:, :kv_width].reshape(length, local_kv, HD)
    value_heads = both[:, kv_width:].reshape(length, local_kv, HD)
    scores = jnp.einsum(
        "qkgd,tkd->kgqt", queries, key_heads, preferred_element_type=F32
    ) / math.sqrt(HD)
    query_positions = me * token_count + jnp.arange(token_count)
    causal = query_positions[:, None] >= key_positions[None, :]
    masked = jnp.where(causal, scores, -1e30)
    row_peak = jnp.max(masked, axis=-1, keepdims=True)
    exp_terms = jnp.where(causal, jnp.exp(masked - row_peak), 0.0)
    weights = (exp_terms / jnp.sum(exp_terms, axis=-1, keepdims=True)).astype(BF)
    context = jnp.einsum("kgqt,tkd->qkgd", weights, value_heads, preferred_element_type=F32)
    return (residual.astype(F32) + context.reshape(token_count, half_width)).astype(BF)


def on_device(query, keys, values, residual, routes, gates, w_gate, w_up, w_down):
    section = lax.axis_index("section")
    hidden = attention(query[0], keys[0], values[0], residual[0])
    token_count, half = hidden.shape
    share = token_count // 2
    experts = w_gate.shape[0]

    def rows_of(value, part):
        return lax.dynamic_slice_in_dim(value, part * share, share, 0)

    gate_high = lax.reduce_precision(gates[0], 8, 7)
    gate_mid = lax.reduce_precision(gates[0] - gate_high, 8, 7)
    gate_low = gates[0] - gate_high - gate_mid
    meta = jnp.concatenate([routes[0].astype(F32), gate_high, gate_mid, gate_low], axis=1)
    meta = jnp.pad(meta, ((0, 0), (0, META - meta.shape[1]))).astype(BF)

    steps = gather_steps()
    sent = rows_of(hidden, 1 - section)
    came = swap(sent, "section", 1)
    x_own = gather_all(rows_of(jnp.concatenate([hidden, meta], axis=1), section), steps)
    x_oth = gather_all(came, steps)

    tokens = x_oth.shape[0]
    info = x_own[:, half : half + 4 * TOP].astype(F32).T
    picked = info[:TOP]
    gate_all = info[TOP : 2 * TOP] + info[2 * TOP : 3 * TOP] + info[3 * TOP : 4 * TOP]
    ids = (lax.axis_index("expert") * experts + jnp.arange(experts)).astype(F32)
    hits = picked[None, :, :] == ids[:, None, None]
    match = jnp.any(hits, axis=1)
    gate = jnp.sum(jnp.where(hits, gate_all[None], 0.0), axis=1)
    lower = jnp.arange(tokens)[:, None] < jnp.arange(tokens)[None, :]
    before = jnp.dot(match.astype(BF), lower.astype(BF), preferred_element_type=F32)
    rank = jnp.where(match, before, -1.0).astype(jnp.int32)
    counts = jnp.sum(match, axis=1).astype(jnp.int32)
    scal = jnp.concatenate([section[None].astype(jnp.int32), counts])
    cap = tokens // share * min(CAP, share)
    main = min(cap, -(-tokens * TOP * 5 // (EXPERTS * 4)) // 16 * 16)

    if tokens <= 1024:
        inner = expert_inner(scal, x_own, x_oth, rank, w_gate, w_up, main, cap)
        pack = (scal, inner, rank, rank.T, gate, w_down)
        sum_oth = expert_outer(*pack, True, main, cap)
        sum_own = expert_outer(*pack, False, main, cap)
    else:
        sum_own, sum_oth = wide_experts(
            section, x_own[:, :half], x_oth, rank, gate, w_gate, w_up, w_down, cap
        )
    sum_oth = scatter_sum(sum_oth, steps)
    partner = swap(sum_oth, "section", 1)
    sum_own = scatter_sum(sum_own, steps)
    first = section == 0
    expert_sum = jnp.concatenate(
        [jnp.where(first, sum_own, partner), jnp.where(first, partner, sum_own)], axis=0
    )
    return (hidden.astype(F32) + expert_sum.astype(F32)).astype(BF)[None]


def solution(mesh):
    return jax.shard_map(
        on_device,
        mesh=mesh,
        in_specs=(
            P("expert", "tensor", "section"),
            P("expert", "tensor", "section"),
            P("expert", "tensor", "section"),
            P("expert", "tensor", "section"),
            P("expert", "tensor", None),
            P("expert", "tensor", None),
            P("expert", None, "tensor"),
            P("expert", None, "tensor"),
            P("expert", "tensor", None),
        ),
        out_specs=P("expert", "tensor", "section"),
        check_vma=False,
    )
```

```python
import functools
import math

import jax
import jax.numpy as jnp
from jax import lax
from jax.experimental import pallas as pl
from jax.experimental.pallas import tpu as pltpu
from jax.sharding import PartitionSpec as P


HD = 128
EXPERTS = 8
TOP = 2
CAP = 17
BF = jnp.bfloat16
F32 = jnp.float32


def swap(value, axis, mask):
    pairs = [(i, i ^ mask) for i in range(lax.axis_size(axis))]
    return lax.ppermute(value, axis, pairs)


def bits_of(axis, lowest):
    count = lax.axis_size(axis).bit_length() - 1
    return [(axis, 1 << b) for b in reversed(range(lowest, count))]


def gather_steps():
    return bits_of("tensor", 1) + bits_of("expert", 0) + [("tensor", 1)]


def named_swap(value, step):
    return swap(value, *step)


def gather_pair(block, steps):
    for step in steps[:-1]:
        block = jnp.concatenate([block, named_swap(block, step)], axis=0)
    return block, named_swap(block, steps[-1])


def gather_four(block, steps, also=()):
    for step in steps[:-2]:
        block = jnp.concatenate([block, named_swap(block, step)], axis=0)
    came = named_swap(block, steps[-2])
    beside = named_swap(block, steps[-1])
    if also:
        beside, also = lax.optimization_barrier((beside, also))
    return (block, came, beside, named_swap(came, steps[-1])), also


def add_rows(a, b):
    return (a.astype(F32) + b.astype(F32)).astype(BF)


def scatter_sum(near, far, steps):
    total = add_rows(near, named_swap(far, steps[-1]))
    for i in reversed(range(len(steps) - 1)):
        half = total.shape[0] // 2
        total = add_rows(total[:half], named_swap(total[half:], steps[i]))
    return total


def hot_rows(rank_row, first, count):
    slots = lax.broadcasted_iota(jnp.int32, (count, rank_row.shape[1]), 0) + first
    return slots == rank_row


def inner_kernel(scal, *refs, main, cap, split, final):
    pieces = refs[:4]
    rank, wg, wu = refs[4:7]
    rest = refs[7:]
    if final:
        (gate_in, up_in, gate_more, up_more), rest = rest[:4], rest[4:]
        out, rows, table = rest
    else:
        gate_out, up_out, gate_spill, up_spill, rows, table = rest
    e, n = pl.program_id(0), pl.program_id(1)

    @pl.when(jnp.logical_and(e == 0, n == 0))
    def _():
        for i, piece in enumerate(pieces):
            table[i * split : (i + 1) * split, :] = piece[...]

    def part(first, count):
        @pl.when(n == 0)
        def _():
            hot = hot_rows(rank[pl.ds(e, 1), :], first, count).astype(BF)
            rows[first : first + count, :] = jnp.dot(
                hot, table[...], preferred_element_type=F32
            ).astype(BF)

        picked = rows[first : first + count, :]
        gate = jnp.dot(picked, wg[0], preferred_element_type=F32)
        up = jnp.dot(picked, wu[0], preferred_element_type=F32)
        if final:
            gate = gate + (gate_more if first else gate_in)[0]
            up = up + (up_more if first else up_in)[0]
            out[0, first : first + count, :] = (gate / (1.0 + jnp.exp(-gate)) * up).astype(BF)
        else:
            (gate_spill if first else gate_out)[0] = gate
            (up_spill if first else up_out)[0] = up

    part(0, main)
    if cap > main:

        @pl.when(scal[1 + e] > main)
        def _():
            part(main, cap - main)


def expert_inner(scal, pieces, rank, w_gate, w_up, partial, main, cap):
    experts, width, hidden = w_gate.shape
    half, split = width // 2, pieces[0].shape[0]
    final = partial is not None
    block = min(1024, hidden)
    more = max(cap - main, 8)

    def spilled(e, s):
        return s[1 + e] > main

    rows_spec = pl.BlockSpec((split, half), lambda e, n, s: (0, 0))
    if final:
        w_spec = pl.BlockSpec((1, half, block), lambda e, n, s: (e, 1 - s[0], n))
    else:
        w_spec = pl.BlockSpec((1, half, block), lambda e, n, s: (e, s[0], n))
    main_spec = pl.BlockSpec((1, main, block), lambda e, n, s: (e, 0, n))
    more_spec = pl.BlockSpec(
        (1, more, block),
        lambda e, n, s: (
            jnp.where(spilled(e, s), e, experts),
            0,
            jnp.where(spilled(e, s), n, 0),
        ),
    )
    partial_specs = [main_spec, main_spec, more_spec, more_spec]
    partial_shapes = [jax.ShapeDtypeStruct((experts, main, hidden), F32)] * 2 + [
        jax.ShapeDtypeStruct((experts + 1, more, hidden), F32)
    ] * 2
    return pl.pallas_call(
        functools.partial(inner_kernel, main=main, cap=cap, split=split, final=final),
        grid_spec=pltpu.PrefetchScalarGridSpec(
            num_scalar_prefetch=1,
            grid=(experts, hidden // block),
            in_specs=[
                rows_spec,
                rows_spec,
                rows_spec,
                rows_spec,
                pl.BlockSpec(rank.shape, lambda e, n, s: (0, 0)),
                w_spec,
                w_spec,
            ]
            + (partial_specs if final else []),
            out_specs=(
                pl.BlockSpec((1, cap, block), lambda e, n, s: (e, 0, n)) if final else partial_specs
            ),
            scratch_shapes=[pltpu.VMEM((cap, half), BF), pltpu.VMEM((4 * split, half), BF)],
        ),
        out_shape=(
            jax.ShapeDtypeStruct((experts, cap, hidden), BF) if final else partial_shapes
        ),
        cost_estimate=pl.CostEstimate(
            flops=4 * experts * main * half * hidden,
            bytes_accessed=4 * experts * half * hidden,
            transcendentals=experts * main * hidden,
        ),
        compiler_params=pltpu.CompilerParams(vmem_limit_bytes=38 << 20),
        name="inner_last" if final else "inner_first",
    )(scal, *pieces, rank, w_gate, w_up, *(partial if final else ()))


def outer_kernel(
    scal, inner, rank, rank_t, gate, wd, near, far, hot, hot_t, slot_gate, total, *, main, cap
):
    experts = wd.shape[0]
    tokens = rank.shape[1]

    def prepare(e, first, count):
        marks = hot_rows(rank[e : e + 1, :], first, count)
        slot_gate[e, first : first + count, :] = jnp.sum(
            jnp.where(marks, gate[e : e + 1, :], 0.0), axis=1, keepdims=True
        )
        lanes = lax.broadcasted_iota(jnp.int32, (tokens, count), 1) + first
        return (lanes == rank_t[:, e : e + 1]).astype(BF)

    def product(e, first, count):
        value = jnp.dot(inner[e, first : first + count, :], wd[e], preferred_element_type=F32)
        return (value * slot_gate[e, first : first + count, :]).astype(BF)

    @pl.when(pl.program_id(0) == 0)
    def _():
        for e in range(experts):
            hot[:, e * main : (e + 1) * main] = prepare(e, 0, main)

    sums = jnp.concatenate([product(e, 0, main) for e in range(experts)], axis=0)
    total[...] = jnp.dot(hot[...], sums, preferred_element_type=F32)
    if cap > main:
        for e in range(experts):

            @pl.when(scal[1 + e] > main)
            def _():
                hot_t[...] = prepare(e, main, cap - main)
                total[...] += jnp.dot(
                    hot_t[...], product(e, main, cap - main), preferred_element_type=F32
                )

    near[...] = total[: tokens // 2, :].astype(BF)
    far[...] = total[tokens // 2 :, :].astype(BF)


def expert_outer(scal, inner, rank, rank_t, gate, w_down, other, main, cap):
    experts, hidden, width = w_down.shape
    half, tokens = width // 2, rank.shape[1]
    block = min(1024, half)
    blocks = half // block
    if other:
        where = lambda n, s: (0, 0, (1 - s[0]) * blocks + n)
    else:
        where = lambda n, s: (0, 0, s[0] * blocks + n)
    out_spec = pl.BlockSpec((tokens // 2, block), lambda n, s: (0, n))
    return pl.pallas_call(
        functools.partial(outer_kernel, main=main, cap=cap),
        grid_spec=pltpu.PrefetchScalarGridSpec(
            num_scalar_prefetch=1,
            grid=(blocks,),
            in_specs=[
                pl.BlockSpec((experts, cap, hidden), lambda n, s: (0, 0, 0)),
                pl.BlockSpec((experts, tokens), lambda n, s: (0, 0)),
                pl.BlockSpec((tokens, experts), lambda n, s: (0, 0)),
                pl.BlockSpec((experts, tokens), lambda n, s: (0, 0)),
                pl.BlockSpec((experts, hidden, block), where),
            ],
            out_specs=[out_spec, out_spec],
            scratch_shapes=[
                pltpu.VMEM((tokens, experts * main), BF),
                pltpu.VMEM((tokens, max(cap - main, 8)), BF),
                pltpu.VMEM((experts, cap, 1), F32),
                pltpu.VMEM((tokens, block), F32),
            ],
        ),
        out_shape=[jax.ShapeDtypeStruct((tokens // 2, half), BF)] * 2,
        cost_estimate=pl.CostEstimate(
            flops=2 * experts * main * (hidden + tokens) * half,
            bytes_accessed=2 * experts * hidden * half,
            transcendentals=0,
        ),
        compiler_params=pltpu.CompilerParams(vmem_limit_bytes=24 << 20),
        name="outer_other" if other else "outer_own",
    )(scal, inner, rank, rank_t, gate, w_down)


def wide_experts(section, x_own, x_oth, rank, gate, w_gate, w_up, w_down, cap):
    half = x_oth.shape[1]
    first = section == 0
    rows = jnp.concatenate(
        [jnp.where(first, x_own, x_oth), jnp.where(first, x_oth, x_own)], axis=1
    )
    tokens, width = rows.shape
    total = jnp.zeros((tokens, width), F32)
    for e in range(w_gate.shape[0]):
        hot = hot_rows(rank[e : e + 1, :], 0, cap)
        slot_gate = jnp.sum(jnp.where(hot, gate[e : e + 1, :], 0.0), axis=1, keepdims=True)
        hot = hot.astype(BF)
        picked = jnp.dot(hot, rows, preferred_element_type=F32).astype(BF)
        g = jnp.dot(picked, w_gate[e], preferred_element_type=F32)
        u = jnp.dot(picked, w_up[e], preferred_element_type=F32)
        inner = (jax.nn.silu(g) * u).astype(BF)
        value = jnp.dot(inner, w_down[e], preferred_element_type=F32)
        value = (value * slot_gate).astype(BF)
        total = total + jnp.dot(hot.T, value, preferred_element_type=F32)
    total = total.astype(BF)
    own = lax.dynamic_slice_in_dim(total, section * half, half, 1)
    oth = lax.dynamic_slice_in_dim(total, (1 - section) * half, half, 1)
    middle = tokens // 2
    return (own[:middle], own[middle:]), (oth[:middle], oth[middle:])


def attention_kernel(start, query, kv0, kv1, key_at, residual, hidden, kv, *, heads, groups):
    rows = query.shape[0]
    split = kv0.shape[0]
    kv[:split, :] = kv0[...]
    kv[split:, :] = kv1[...]
    at = lax.rem(lax.broadcasted_iota(jnp.int32, (groups * rows, kv.shape[0]), 0), rows) + start[0]
    causal = at >= key_at[...]
    for head in range(heads):
        first = head * groups
        wanted = jnp.concatenate(
            [query[:, (first + g) * HD : (first + g + 1) * HD] for g in range(groups)], axis=0
        )
        scores = lax.dot_general(
            wanted,
            kv[:, head * HD : (head + 1) * HD],
            (((1,), (1,)), ((), ())),
            preferred_element_type=F32,
        ) / math.sqrt(HD)
        masked = jnp.where(causal, scores, -1e30)
        peak = jnp.max(masked, axis=1, keepdims=True)
        terms = jnp.where(causal, jnp.exp(masked - peak), 0.0)
        weights = (terms / jnp.sum(terms, axis=1, keepdims=True)).astype(BF)
        context = jnp.dot(
            weights,
            kv[:, (heads + head) * HD : (heads + head + 1) * HD],
            preferred_element_type=F32,
        )
        for g in range(groups):
            cols = slice((first + g) * HD, (first + g + 1) * HD)
            hidden[:, cols] = (
                residual[:, cols].astype(F32) + context[g * rows : (g + 1) * rows, :]
            ).astype(BF)


def attention(query, keys, values, residual, info):
    token_count, half_width = query.shape
    kv_width = keys.shape[1]
    steps = bits_of("tensor", 0)
    pieces = gather_pair(jnp.concatenate([keys, values], axis=1), steps)
    pieces = lax.optimization_barrier((*pieces, info))[:2]
    me = lax.axis_index("tensor")
    order = [0]
    for axis, mask in steps:
        order = order + [j ^ mask for j in order]
    source = me ^ jnp.array(order, jnp.int32)
    key_at = (source[:, None] * token_count + jnp.arange(token_count)[None, :]).reshape(1, -1)
    length = key_at.shape[1]
    groups = half_width // kv_width
    full = pl.BlockSpec(memory_space=pltpu.VMEM)
    return pl.pallas_call(
        functools.partial(attention_kernel, heads=kv_width // HD, groups=groups),
        in_specs=[pl.BlockSpec(memory_space=pltpu.SMEM)] + [full] * 5,
        out_specs=full,
        out_shape=jax.ShapeDtypeStruct((token_count, half_width), BF),
        scratch_shapes=[pltpu.VMEM((length, 2 * kv_width), BF)],
        cost_estimate=pl.CostEstimate(
            flops=4 * token_count * length * half_width,
            bytes_accessed=8 * token_count * half_width,
            transcendentals=token_count * length * half_width // HD,
        ),
        compiler_params=pltpu.CompilerParams(vmem_limit_bytes=16 << 20),
        name="attention",
    )((me * token_count)[None].astype(jnp.int32), query, *pieces, key_at, residual)


def on_device(query, keys, values, residual, routes, gates, w_gate, w_up, w_down):
    section = lax.axis_index("section")
    token_count, _ = query[0].shape
    share = token_count // 2
    experts = w_gate.shape[0]

    def rows_of(value, part):
        return lax.dynamic_slice_in_dim(value, part * share, share, 0)

    steps = gather_steps()
    info = jnp.concatenate([routes[0].astype(F32), gates[0]], axis=1)
    info = jnp.concatenate(gather_pair(rows_of(info, section), steps), axis=0)
    hidden = attention(query[0], keys[0], values[0], residual[0], info)
    sent = rows_of(hidden, 1 - section)
    came = named_swap(sent, ("section", 1))
    tokens = info.shape[0]
    ids = (lax.axis_index("expert") * experts + jnp.arange(experts)).astype(F32)
    order = jnp.arange(tokens)
    lines = info.T
    hits = lines[:TOP][None] == ids[:, None, None]
    match = jnp.any(hits, axis=1)
    gate_all = lines[TOP:]
    gate = jnp.sum(jnp.where(hits, gate_all[None], 0.0), axis=1)
    lower = (order[:, None] < order[None, :]).astype(BF)
    before = jnp.dot(match.astype(BF), lower, preferred_element_type=F32)
    rank = jnp.where(match, before, -1.0).astype(jnp.int32)
    match_t = jnp.any(info[:, :TOP][:, :, None] == ids[None, None, :], axis=1)
    upper = (order[:, None] > order[None, :]).astype(BF)
    before_t = jnp.dot(upper, match_t.astype(BF), preferred_element_type=F32)
    rank_t = jnp.where(match_t, before_t, -1.0).astype(jnp.int32)
    counts = jnp.sum(match, axis=1).astype(jnp.int32)
    scal = jnp.concatenate([section[None].astype(jnp.int32), counts])
    cap = tokens // share * min(CAP, share)
    main = min(cap, -(-tokens * TOP * 5 // (EXPERTS * 4)) // 16 * 16)

    table = (scal, rank, rank_t, gate)
    own, (scal, rank, rank_t, gate) = gather_four(rows_of(hidden, section), steps, table)
    oth, _ = gather_four(came, steps)
    if tokens <= 1024:
        partial = expert_inner(scal, own, rank, w_gate, w_up, None, main, cap)
        inner = expert_inner(scal, oth, rank, w_gate, w_up, partial, main, cap)
        pack = (scal, inner, rank, rank_t, gate, w_down)
        sum_oth = expert_outer(*pack, True, main, cap)
        sum_own = expert_outer(*pack, False, main, cap)
    else:
        x_own = jnp.concatenate(own, axis=0)
        x_oth = jnp.concatenate(oth, axis=0)
        sum_own, sum_oth = wide_experts(
            section, x_own, x_oth, rank, gate, w_gate, w_up, w_down, cap
        )
    sum_oth = scatter_sum(*sum_oth, steps)
    partner = named_swap(sum_oth, ("section", 1))
    sum_own = scatter_sum(*sum_own, steps)
    first = section == 0
    expert_sum = jnp.concatenate(
        [jnp.where(first, sum_own, partner), jnp.where(first, partner, sum_own)], axis=0
    )
    return (hidden.astype(F32) + expert_sum.astype(F32)).astype(BF)[None]


def solution(mesh):
    last = len([n for n in ("expert",) for _ in range(mesh.shape[n].bit_length() - 1)])
    last += mesh.shape["tensor"].bit_length() - 2
    return jax.shard_map(
        on_device,
        mesh=mesh,
        in_specs=(
            P("expert", "tensor", "section"),
            P("expert", "tensor", "section"),
            P("expert", "tensor", "section"),
            P("expert", "tensor", "section"),
            P("expert", "tensor", None),
            P("expert", "tensor", None),
            P("expert", None, "tensor"),
            P("expert", None, "tensor"),
            P("expert", "tensor", None),
        ),
        out_specs=P("expert", "tensor", "section"),
        check_vma=False,
    )
```
